32 devices in a mesh: row: 4 (over y, x), col: 8 (over z, core).
Axes of the slice: x: 2, y: 2, z: 4, core: 2. Of those that a mesh axis runs over, the one named last changes fastest.
Arguments:
- vorticity: float32 [3, 128, 128, 128], P(None, 'row', 'col'), may hold values from -18.1 to 18.1
- scalar: float32 [256, 256, 256], P('row', 'col'), may hold values from -6 to 6
Outputs:
- advected: float32 [256, 256, 256], P('row', 'col')
The draws below stay inside these ranges and needn't reach their ends.
All inputs are finite; a program needn't handle non-finite values. Where the reference program divides by a largest or mean magnitude, that divisor is 1e-20 or more.
Results may differ from the reference program's by a relative error of at most 0.0003.
Values sent between devices are 32-bit elements; how exact they have to be, the bound alone decides.
A program may use at most 128 MiB of HBM per device.

```python
import jax
import jax.numpy as jnp

N = 128
NF = 256


def draw_vorticity(key, part):
    coords = jnp.arange(N, dtype=jnp.float32) / (N - 1.0)
    ramp = 0.5 * (coords[:, None] + coords[None, :])
    spread = jnp.exp(jnp.log(3.0) * ramp)
    noise = jnp.clip(jax.random.normal(key, (3, N, N, N), jnp.float32), -6.0, 6.0)
    return noise * spread[None, :, :, None]


def block_scale(rng, dims, cuts, low, high):
    loudness, own = 1.0, jax.random.fold_in(rng, 6)
    for position, blocks in cuts:
        steps = jnp.exp(jax.random.uniform(jax.random.fold_in(own, position), (blocks,), jnp.float32, low / len(cuts), high / len(cuts)))
        loudness = loudness * jnp.repeat(steps, dims[position] // blocks).reshape([-1 if axis == position else 1 for axis in range(len(dims))])
    return loudness


def bell_draw(own_key, shape, scale, limit, shards=(), kind=jnp.bfloat16):
    values = scale * jax.random.normal(own_key, shape, jnp.float32)
    if shards:
        values = values * block_scale(own_key, shape, shards, -0.22, 0.18)
    return jnp.clip(values, -limit, limit).astype(kind)


def setup_inputs(seed: int = 0) -> dict:
    key_list = jax.random.split(jax.random.key(seed), 3)
    return {
        "vorticity": draw_vorticity(jax.random.fold_in(key_list[2], 71), 0),
        "scalar": bell_draw(key_list[1], (NF, NF, NF), 1.0, 6.0, ((0, 4), (1, 8)), jnp.float32),
    }


COURANT = 0.9
EPSILON = 1e-6


def kernel_weight(distance):
    radius = jnp.abs(distance)
    inner_lobe = -(radius - 1.0) * ((((25.0 * radius - 38.0) * radius - 3.0) * radius + 12.0) * radius + 12.0) / 12.0
    middle_lobe = (radius - 1.0) * (radius - 2.0) * (((25.0 * radius - 114.0) * radius + 153.0) * radius - 48.0) / 24.0
    outer_cube = (radius - 3.0) * (radius - 3.0) * (radius - 3.0)
    outer_lobe = -(radius - 2.0) * outer_cube * (5.0 * radius - 8.0) / 24.0
    return jnp.where(radius < 1.0, inner_lobe, jnp.where(radius < 2.0, middle_lobe, jnp.where(radius < 3.0, outer_lobe, 0.0)))


def induce(vorticity):
    spectrum = jnp.fft.fftn(vorticity, axes=(1, 2, 3))
    indices = jnp.arange(N, dtype=jnp.int32)
    waves = jnp.where(indices < N // 2, indices, indices - N).astype(jnp.float32)
    nyquist = indices == N // 2
    ywaves = waves[:, None, None]
    zwaves = waves[None, :, None]
    xwaves = waves[None, None, :]
    wave_sq = xwaves * xwaves + ywaves * ywaves + zwaves * zwaves
    banned = nyquist[:, None, None] | nyquist[None, :, None] | nyquist[None, None, :]
    keep = (wave_sq > 0.0) & jnp.logical_not(banned)
    factor = jnp.where(keep, 1.0 / jnp.maximum(wave_sq, 1.0), 0.0)
    cross = jnp.stack([ywaves * spectrum[2] - zwaves * spectrum[1],
                       zwaves * spectrum[0] - xwaves * spectrum[2],
                       xwaves * spectrum[1] - ywaves * spectrum[0]])
    velocity_hat = 1j * cross * factor
    return jnp.real(jnp.fft.ifftn(velocity_hat, axes=(1, 2, 3))).astype(jnp.float32)


def refine(coarse, grid_axis):
    lower = 0.75 * coarse + 0.25 * jnp.roll(coarse, 1, grid_axis)
    upper = 0.75 * coarse + 0.25 * jnp.roll(coarse, -1, grid_axis)
    shape = list(coarse.shape)
    shape[grid_axis] = 2 * shape[grid_axis]
    return jnp.stack([lower, upper], axis=grid_axis + 1).reshape(shape)


def remesh(field, displace, grid_axis):
    summed = jnp.zeros(field.shape, jnp.float32)
    for offset in range(-3, 4):
        summed = summed + jnp.roll(field, offset, grid_axis) * kernel_weight(offset - jnp.roll(displace, offset, grid_axis))
    return summed


def reference(vorticity, scalar):
    velocity = induce(vorticity)
    velocity_peak = jnp.max(jnp.abs(velocity))
    courant_scale = COURANT / (velocity_peak + EPSILON)
    result = scalar
    for component, grid_axis in ((0, 2), (1, 0), (2, 1)):
        fine = refine(refine(refine(velocity[component], 2), 0), 1) * courant_scale
        result = remesh(result, fine, grid_axis)
    return result
```

```python
import functools

import jax
import jax.numpy as jnp
import numpy as np
from jax import lax
from jax.experimental import pallas as pl
from jax.experimental.pallas import tpu as pltpu
from jax.sharding import PartitionSpec as P

COURANT = 0.9
EPSILON = 1e-06
HIGHEST = lax.Precision.HIGHEST
MESH = pl.DeviceIdType.MESH


def refine_matrix(n):
    matrix = np.zeros((2 * n, n))
    for j in range(n):
        matrix[2 * j, j] += 0.75
        matrix[2 * j, (j - 1) % n] += 0.25
        matrix[2 * j + 1, j] += 0.75
        matrix[2 * j + 1, (j + 1) % n] += 0.25
    return matrix


def tables(n, rows, padded):
    index = np.arange(n)
    angle = 2.0 * np.pi * (index[:, None] * index[None, :] % n) / n
    cos, sin = np.cos(angle), np.sin(angle)
    half = n // 2
    forward_x = np.concatenate([cos[:, :half], -sin[:, :half]], axis=1)
    weight = np.where(index[:half] == 0, 1.0, 2.0)[:, None]
    back = np.concatenate([cos[:half] * weight, -sin[:half] * weight], axis=0)
    back_x = np.concatenate([back @ refine_matrix(n).T, back], axis=1)
    both = np.concatenate([cos, sin], axis=0)
    count = n // rows
    picked = np.zeros((2, rows, padded, n))
    for r in range(rows):
        lines = [r * count + i for i in range(count)] + [(r * count - 1) % n, (r * count + count) % n]
        picked[0, r, : count + 2] = cos[lines]
        picked[1, r, : count + 2] = sin[lines]
    inverse_y = picked.reshape(2 * rows * padded, n)
    return [t.astype(np.float32) for t in (forward_x, both, inverse_y, back_x)]


def dot(a, b):
    return jnp.dot(a, b, precision=HIGHEST, preferred_element_type=jnp.float32)


def spread(field, displace):
    a = jnp.abs(displace)
    b = 1.0 - a
    q = field * (a * b) * (1.0 / 24.0)
    p3 = q * (a * a) * (7.0 - 5.0 * a)
    m2 = q * (b * b) * (7.0 - 5.0 * b)
    p2 = q * (((25.0 * a - 36.0) * a - 3.0) * a - 2.0 - 0.0)
    m1 = q * (((25.0 * b - 36.0) * b - 3.0) * b - 2.0 - 0.0)
    p1 = field * a - 2.0 * p2 - 3.0 * p3 + m1 + 2.0 * m2
    c0 = field - p1 - p2 - p3 - m1 - m2
    up = displace >= 0.0
    zero = jnp.zeros_like(p3)
    return {
        0: c0,
        1: jnp.where(up, p1, m1),
        -1: jnp.where(up, m1, p1),
        2: jnp.where(up, p2, m2),
        -2: jnp.where(up, m2, p2),
        3: jnp.where(up, p3, zero),
        -3: jnp.where(up, zero, p3),
    }


def body(
    rows, cols, jrows,
    vort, scalar, fx, both, iy, bx, out,
    tmp, g1, r1, s2, r2, s3, r3, w4, r4, fine, peaks, pack, disp_z, acc, halo_y, zr, zl, zin_r, zin_l,
    sem1, sem2, sem3, sem4, sem4h, semp, semy, semz,
):
    n = vort.shape[2]
    ny, nz = n // rows, n // cols
    zc = nz // rows
    devices = rows * cols
    kc = n // devices
    chunk = zc * jrows
    padded = ny + 8
    zp = fine.shape[1] // (ny + 2)
    nf, nzf = 2 * ny, 2 * nz
    half = n // 2
    row, col = lax.axis_index("row"), lax.axis_index("col")
    me = col * rows + row

    def where_is(index):
        return (lax.rem(index, rows), index // rows)

    barrier = pltpu.get_barrier_semaphore()

    def greet(p, carry):
        pl.semaphore_signal(barrier, inc=1, device_id=where_is(lax.rem(me + p, devices)), device_id_type=MESH)
        return carry

    lax.fori_loop(1, devices, greet, 0)

    lane = lax.broadcasted_iota(jnp.int32, (1, n), 1)
    sign = jnp.where(lane < half, 1.0, -1.0)

    def turn(product, direction):
        count = product.shape[0] // 2
        swapped = pltpu.roll(product[count:], half, axis=1)
        return product[:count] + swapped * (sign * direction)

    for c in range(3):
        tmp[c] = dot(vort[c], fx[...])
    for z in range(nz):
        for c in range(3):
            g1[z // zc, pl.ds(((z % zc) * 3 + c) * ny, ny), :] = tmp[c, pl.ds(z, ny, stride=nz), :]
    pl.semaphore_wait(barrier, devices - 1)

    def copy_row(source, target, sems, p):
        peer = lax.rem(row + p, rows)
        return pltpu.make_async_remote_copy(
            src_ref=source.at[peer], dst_ref=target.at[row], send_sem=sems.at[0, p], recv_sem=sems.at[1, p],
            device_id=(peer, col), device_id_type=MESH)

    first = [copy_row(g1, r1, sem1, p) for p in range(1, rows)]
    for copy in first:
        copy.start()
    r1[row] = g1[row]
    for copy in first:
        copy.wait()

    for z in range(zc):
        for c in range(3):
            lines = jnp.concatenate([r1[r, pl.ds((z * 3 + c) * ny, ny), :] for r in range(rows)], axis=0)
            modes = turn(dot(both[...], lines), 1.0)
            for k in range(kc):
                s2[pl.ds(z * jrows + k * 3 + c, devices, stride=chunk), :] = modes[k * devices:(k + 1) * devices]

    def exchange(source, target, sems):
        def make(p):
            peer = lax.rem(me + p, devices)
            return pltpu.make_async_remote_copy(
                src_ref=source.at[pl.ds(pl.multiple_of(peer * chunk, 8), chunk)],
                dst_ref=target.at[pl.ds(pl.multiple_of(me * chunk, 8), chunk)],
                send_sem=sems.at[0, p], recv_sem=sems.at[1, p],
                device_id=where_is(peer), device_id_type=MESH)

        def start(p, carry):
            make(p).start()
            return carry

        def wait(p, carry):
            make(p).wait()
            return carry

        lax.fori_loop(1, devices, start, 0)
        own = pl.ds(pl.multiple_of(me * chunk, 8), chunk)
        target[own, :] = source[own, :]
        lax.fori_loop(1, devices, wait, 0)

    exchange(s2, r2, sem2)

    xi = lax.broadcasted_iota(jnp.int32, (n, n), 1)
    zi = lax.broadcasted_iota(jnp.int32, (n, n), 0)
    kx = jnp.where(xi < half, xi, xi - half).astype(jnp.float32)
    kz = jnp.where(zi < half, zi, zi - n).astype(jnp.float32)
    for k in range(kc):
        yi = k * devices + me
        ky_int = yi - jnp.where(yi < half, 0, n)
        ky = jnp.full((n, n), ky_int, jnp.int32).astype(jnp.float32)
        square = kx * kx + ky * ky + kz * kz
        keep = (square > 0.0) & (zi != half) & (jnp.full((n, n), yi, jnp.int32) != half)
        factor = jnp.where(keep, 1.0 / jnp.maximum(square, 1.0), 0.0) * (1.0 / (n * n * n))
        ox, oy, oz = [turn(dot(both[...], r2[pl.ds(k * 3 + c, n, stride=jrows), :]), 1.0) for c in range(3)]
        for c, cross in enumerate((ky * oz - kz * oy, kz * ox - kx * oz, kx * oy - ky * ox)):
            hat = pltpu.roll(cross * factor, half, axis=1) * (-sign)
            s3[pl.ds(k * 3 + c, n, stride=jrows), :] = turn(dot(both[...], hat), -1.0)

    exchange(s3, r3, sem3)

    for z in range(zc):
        for c in range(3):
            modes = jnp.concatenate(
                [r3[pl.ds(z * jrows + k * 3 + c, devices, stride=chunk), :] for k in range(kc)], axis=0)
            lines = turn(dot(iy[...], modes), -1.0)
            for r in range(rows):
                w4[r, z, pl.ds(c * padded, padded), :] = lines[r * padded:(r + 1) * padded]

    def copy_back(p):
        peer = lax.rem(row + p, rows)
        return pltpu.make_async_remote_copy(
            src_ref=w4.at[peer], dst_ref=r4.at[pl.ds(1 + row * zc, zc)], send_sem=sem4.at[0, p],
            recv_sem=sem4.at[1, p], device_id=(peer, col), device_id_type=MESH)

    def copy_layer(r, top):
        step = 1 if top else cols - 1
        return pltpu.make_async_remote_copy(
            src_ref=w4.at[r, zc - 1 if top else 0], dst_ref=r4.at[0 if top else nz + 1],
            send_sem=sem4h.at[0 if top else 1, r], recv_sem=sem4h.at[0 if top else 1, rows],
            device_id=(r, lax.rem(col + step, cols)), device_id_type=MESH)

    @pl.when(row == rows - 1)
    def _():
        for r in range(rows):
            copy_layer(r, True).start()

    @pl.when(row == 0)
    def _():
        for r in range(rows):
            copy_layer(r, False).start()

    last = [copy_back(p) for p in range(1, rows)]
    for copy in last:
        copy.start()
    r4[pl.ds(1 + row * zc, zc)] = w4[row]
    for copy in last:
        copy.wait()
    copy_layer(0, True).wait_recv()
    copy_layer(0, False).wait_recv()

    @pl.when(row == rows - 1)
    def _():
        for r in range(rows):
            copy_layer(r, True).wait_send()

    @pl.when(row == 0)
    def _():
        for r in range(rows):
            copy_layer(r, False).wait_send()

    top = jnp.zeros((8, n), jnp.float32)
    for z in range(nz + 2):
        product = dot(r4[z], bx[...])
        size = jnp.abs(product[:, 2 * n:])
        top = jnp.maximum(top, jnp.max(size.reshape(size.shape[0] // 8, 8, n), axis=0))
        for c in range(3):
            for h in range(2):
                part = product[c * padded:(c + 1) * padded, h * n:(h + 1) * n]
                fine[c * 2 + h, pl.ds(zp + z, ny, stride=zp), :] = part[:ny]
                fine[c * 2 + h, pl.ds(z, 1), :] = part[ny:ny + 1]
                fine[c * 2 + h, pl.ds((ny + 1) * zp + z, 1), :] = part[ny + 1:ny + 2]
    peaks[me] = top

    def send_peak(p):
        return pltpu.make_async_remote_copy(
            src_ref=peaks.at[me], dst_ref=peaks.at[me], send_sem=semp.at[0, p], recv_sem=semp.at[1, p],
            device_id=where_is(lax.rem(me + p, devices)), device_id_type=MESH)

    def peak_start(p, carry):
        send_peak(p).start()
        return carry

    def peak_wait(p, carry):
        send_peak(p).wait()
        return carry

    lax.fori_loop(1, devices, peak_start, 0)

    def clear(y, carry):
        acc[y] = jnp.zeros((nzf, 2 * n), jnp.float32)
        return carry

    lax.fori_loop(0, nf + 6, clear, 0)
    lax.fori_loop(1, devices, peak_wait, 0)
    scale = COURANT / (jnp.max(peaks[...]) + EPSILON)

    def sweep(j):
        def plane(ch, y):
            return fine[ch, pl.ds(pl.multiple_of(y * zp, 8), zp), :]

        for c in range(3):
            for h in range(2):
                middle = plane(c * 2 + h, j + 1) * (0.75 * scale)
                for side in range(2):
                    line = middle + plane(c * 2 + h, j + 2 * side) * (0.25 * scale)
                    inner = 0.75 * line[1:nz + 1]
                    pack[side * 6 + c * 2 + h, pl.ds(0, nz, stride=2), :] = inner + 0.25 * line[0:nz]
                    pack[side * 6 + c * 2 + h, pl.ds(1, nz, stride=2), :] = inner + 0.25 * line[2:nz + 2]
        for side in range(2):
            y = 2 * j + side
            dx, dy, dz = [
                jnp.concatenate([pack[side * 6 + c * 2], pack[side * 6 + c * 2 + 1]], axis=1) for c in range(3)]
            disp_z[y] = dz
            parts = spread(scalar[y], dx)
            swept = parts[0]
            for offset in (1, 2, 3):
                swept = swept + pltpu.roll(parts[offset], offset, axis=1)
                swept = swept + pltpu.roll(parts[-offset], 2 * n - offset, axis=1)
            parts = spread(swept, dy)
            for offset in range(-3, 4):
                acc[y + 3 + offset] += parts[offset]

    def edge(i):
        return jnp.where(i < 2, i, ny - 4 + i)

    def sweep_edge(i, carry):
        sweep(edge(i))
        return carry

    def sweep_inner(j, carry):
        sweep(j)
        return carry

    lax.fori_loop(0, 4, sweep_edge, 0)

    def copy_y(up):
        step = 1 if up else rows - 1
        side = 0 if up else 1
        return pltpu.make_async_remote_copy(
            src_ref=acc.at[pl.ds(nf + 3 if up else 0, 3)], dst_ref=halo_y.at[side], send_sem=semy.at[0, side],
            recv_sem=semy.at[1, side], device_id=(lax.rem(row + step, rows), col), device_id_type=MESH)

    copy_y(True).start()
    copy_y(False).start()
    lax.fori_loop(2, ny - 2, sweep_inner, 0)

    row_of = lax.broadcasted_iota(jnp.int32, (nzf, 2 * n), 0)
    row8 = lax.broadcasted_iota(jnp.int32, (8, 2 * n), 0)

    def lift(p):
        tiles = []
        for side in range(2):
            y = 2 * p + side
            parts = spread(acc[y + 3], disp_z[y])
            kept = parts[0]
            above = jnp.zeros((8, 2 * n), jnp.float32)
            below = jnp.zeros((8, 2 * n), jnp.float32)
            for offset in (1, 2, 3):
                moved = pltpu.roll(parts[offset], offset, axis=0)
                kept = kept + jnp.where(row_of >= offset, moved, 0.0)
                above = above + jnp.where(row8 < offset, moved[:8], 0.0)
                moved = pltpu.roll(parts[-offset], nzf - offset, axis=0)
                kept = kept + jnp.where(row_of < nzf - offset, moved, 0.0)
                below = below + jnp.where(row8 >= 8 - offset, moved[nzf - 8:], 0.0)
            out[y] = kept
            tiles.append((above, below))
        zr[p] = tiles[0][0] + pltpu.roll(tiles[1][0], 4, axis=0)
        zl[p] = tiles[0][1] + pltpu.roll(tiles[1][1], 4, axis=0)

    def lift_inner(p, carry):
        lift(p)
        return carry

    def lift_edge(i, carry):
        lift(edge(i))
        return carry

    def copy_z(index):
        start, count = ((2, ny - 4), (0, 2), (ny - 2, 2))[index]
        here = pl.ds(start, count)
        return [
            pltpu.make_async_remote_copy(
                src_ref=source.at[here], dst_ref=target.at[here], send_sem=semz.at[0, side, index],
                recv_sem=semz.at[1, side, index], device_id=(row, lax.rem(col + step, cols)), device_id_type=MESH)
            for side, source, target, step in ((0, zr, zin_r, 1), (1, zl, zin_l, cols - 1))]

    lax.fori_loop(2, ny - 2, lift_inner, 0)
    for copy in copy_z(0):
        copy.start()
    copy_y(True).wait()
    copy_y(False).wait()
    for i in range(3):
        acc[3 + i] += halo_y[0, i]
        acc[nf + i] += halo_y[1, i]
    lax.fori_loop(0, 4, lift_edge, 0)
    for index in (1, 2):
        for copy in copy_z(index):
            copy.start()

    def finish(p, carry):
        low, high = zin_r[p], zin_l[p]
        for side in range(2):
            if side:
                low, high = pltpu.roll(low, 4, axis=0), pltpu.roll(high, 4, axis=0)
            out[2 * p + side, :8, :] += jnp.where(row8 < 3, low, 0.0)
            out[2 * p + side, nzf - 8:, :] += jnp.where(row8 >= 5, high, 0.0)
        return carry

    for index, (start, stop) in enumerate(((2, ny - 2), (0, 2), (ny - 2, ny))):
        for copy in copy_z(index):
            copy.wait()
        lax.fori_loop(start, stop, finish, 0)


def shards(rows, cols, vorticity, scalar):
    n = vorticity.shape[3]
    ny, nz = vorticity.shape[1], vorticity.shape[2]
    devices = rows * cols
    zc, kc = nz // rows, n // devices
    jrows = kc * 3
    while zc * jrows % 8:
        jrows += 1
    padded = ny + 8
    zp = (nz + 2 + 7) // 8 * 8
    nf, nzf = 2 * ny, 2 * nz
    f32 = jnp.float32
    total = devices * zc * jrows
    vmem = pl.BlockSpec(memory_space=pltpu.VMEM)
    dma = pltpu.SemaphoreType.DMA
    return pl.pallas_call(
        functools.partial(body, rows, cols, jrows),
        out_shape=jax.ShapeDtypeStruct((nf, nzf, 2 * n), f32),
        in_specs=[vmem] * 6,
        out_specs=vmem,
        scratch_shapes=[
            pltpu.VMEM((3, ny * nz, n), f32),
            pltpu.VMEM((rows, zc * 3 * ny, n), f32),
            pltpu.VMEM((rows, zc * 3 * ny, n), f32),
            pltpu.VMEM((total, n), f32),
            pltpu.VMEM((total, n), f32),
            pltpu.VMEM((total, n), f32),
            pltpu.VMEM((total, n), f32),
            pltpu.VMEM((rows, zc, 3 * padded, n), f32),
            pltpu.VMEM((nz + 2, 3 * padded, n), f32),
            pltpu.VMEM((6, (ny + 2) * zp, n), f32),
            pltpu.VMEM((devices, 8, n), f32),
            pltpu.VMEM((12, nzf, n), f32),
            pltpu.VMEM((nf, nzf, 2 * n), f32),
            pltpu.VMEM((nf + 6, nzf, 2 * n), f32),
            pltpu.VMEM((2, 3, nzf, 2 * n), f32),
            pltpu.VMEM((ny, 8, 2 * n), f32),
            pltpu.VMEM((ny, 8, 2 * n), f32),
            pltpu.VMEM((ny, 8, 2 * n), f32),
            pltpu.VMEM((ny, 8, 2 * n), f32),
            dma((2, rows)),
            dma((2, devices)),
            dma((2, devices)),
            dma((2, rows)),
            dma((2, rows + 1)),
            dma((2, devices)),
            dma((2, 2)),
            dma((2, 2, 3)),
        ],
        compiler_params=pltpu.CompilerParams(
            collective_id=0, has_side_effects=True, vmem_limit_bytes=56 * 1024 * 1024),
    )(vorticity.reshape(3, ny * nz, n), scalar, *[jnp.asarray(t) for t in tables(n, rows, padded)])


def solution(mesh):
    rows, cols = mesh.shape["row"], mesh.shape["col"]
    return jax.shard_map(
        functools.partial(shards, rows, cols),
        mesh=mesh,
        in_specs=(P(None, "row", "col", None), P("row", "col", None)),
        out_specs=P("row", "col", None),
        check_vma=False,
    )
```

```python
import functools

import jax
import jax.numpy as jnp
import numpy as np
from jax import lax
from jax.experimental import pallas as pl
from jax.experimental.pallas import tpu as pltpu
from jax.sharding import PartitionSpec as P

COURANT = 0.9
EPSILON = 1e-06
HIGH = lax.Precision.HIGH
MESH = pl.DeviceIdType.MESH


def refine_matrix(n):
    matrix = np.zeros((2 * n, n))
    for j in range(n):
        matrix[2 * j, j] += 0.75
        matrix[2 * j, (j - 1) % n] += 0.25
        matrix[2 * j + 1, j] += 0.75
        matrix[2 * j + 1, (j + 1) % n] += 0.25
    return matrix


def tables(n, rows, padded):
    index = np.arange(n)
    angle = 2.0 * np.pi * (index[:, None] * index[None, :] % n) / n
    cos, sin = np.cos(angle), np.sin(angle)
    half = n // 2
    forward_x = np.concatenate([cos[:, :half], -sin[:, :half]], axis=1)
    weight = np.where(index[:half] == 0, 1.0, 2.0)[:, None]
    back = np.concatenate([cos[:half] * weight, -sin[:half] * weight], axis=0)
    back_x = np.concatenate([back @ refine_matrix(n).T, back], axis=1)
    both = np.concatenate([cos, sin], axis=0)
    count = n // rows
    picked = np.zeros((2, rows, padded, n))
    for r in range(rows):
        lines = [r * count + i for i in range(count)] + [(r * count - 1) % n, (r * count + count) % n]
        picked[0, r, : count + 2] = cos[lines]
        picked[1, r, : count + 2] = sin[lines]
    inverse_y = picked.reshape(2 * rows * padded, n)
    return [t.astype(np.float32) for t in (forward_x, both, inverse_y, back_x)]


def dot(a, b):
    return jnp.dot(a, b, precision=HIGH, preferred_element_type=jnp.float32)


def spread(field, displace):
    a = jnp.abs(displace)
    b = 1.0 - a
    q = field * (a * b) * (1.0 / 24.0)
    p3 = q * (a * a) * (7.0 - 5.0 * a)
    m2 = q * (b * b) * (7.0 - 5.0 * b)
    p2 = q * (((25.0 * a - 36.0) * a - 3.0) * a - 2.0 - 0.0)
    m1 = q * (((25.0 * b - 36.0) * b - 3.0) * b - 2.0 - 0.0)
    p1 = field * a - 2.0 * p2 - 3.0 * p3 + m1 + 2.0 * m2
    c0 = field - p1 - p2 - p3 - m1 - m2
    up = displace >= 0.0
    zero = jnp.zeros_like(p3)
    return {
        0: c0,
        1: jnp.where(up, p1, m1),
        -1: jnp.where(up, m1, p1),
        2: jnp.where(up, p2, m2),
        -2: jnp.where(up, m2, p2),
        3: jnp.where(up, p3, zero),
        -3: jnp.where(up, zero, p3),
    }


def body(
    rows, cols, jrows,
    vort, scalar, fx, both, iy, bx, out,
    tmp, g1, r1, s2, r2, omega, factor, s3, r3, w4, r4, fine, peaks, pack, disp_z, acc, halo_y, zr, zl, zin_r, zin_l,
    sem1, sem2, sem3, sem4, sem4h, semp, semy, semz,
):
    n = vort.shape[2]
    ny, nz = n // rows, n // cols
    zc = nz // rows
    devices = rows * cols
    kc = n // devices
    chunk = zc * jrows
    padded = ny + 8
    zp = fine.shape[1] // (ny + 2)
    nf, nzf = 2 * ny, 2 * nz
    half = n // 2
    row, col = lax.axis_index("row"), lax.axis_index("col")
    me = col * rows + row

    def where_is(index):
        return (lax.rem(index, rows), index // rows)

    barrier = pltpu.get_barrier_semaphore()

    def greet(p, carry):
        pl.semaphore_signal(barrier, inc=1, device_id=where_is(lax.rem(me + p, devices)), device_id_type=MESH)
        return carry

    lax.fori_loop(1, devices, greet, 0)

    lane = lax.broadcasted_iota(jnp.int32, (1, n), 1)
    sign = jnp.where(lane < half, 1.0, -1.0)

    def turn(product, direction):
        count = product.shape[0] // 2
        swapped = pltpu.roll(product[count:], half, axis=1)
        return product[:count] + swapped * (sign * direction)

    def copy_row(c, p):
        peer = lax.rem(row + p, rows)
        return pltpu.make_async_remote_copy(
            src_ref=g1.at[c, peer], dst_ref=r1.at[c, row], send_sem=sem1.at[0, c, p], recv_sem=sem1.at[1, c, p],
            device_id=(peer, col), device_id_type=MESH)

    for c in range(3):
        tmp[c] = dot(vort[c], fx[...])
        for z in range(nz):
            g1[c, z // zc, pl.ds((z % zc) * ny, ny), :] = tmp[c, pl.ds(z, ny, stride=nz), :]
        if c == 0:
            pl.semaphore_wait(barrier, devices - 1)
        for p in range(1, rows):
            copy_row(c, p).start()
        r1[c, row] = g1[c, row]

    def make(source, target, sems, c, p):
        peer = lax.rem(me + p, devices)
        return pltpu.make_async_remote_copy(
            src_ref=source.at[c, pl.ds(pl.multiple_of(peer * chunk, 8), chunk)],
            dst_ref=target.at[c, pl.ds(pl.multiple_of(me * chunk, 8), chunk)],
            send_sem=sems.at[0, c, p], recv_sem=sems.at[1, c, p],
            device_id=where_is(peer), device_id_type=MESH)

    def send(source, target, sems, c):
        def start(p, carry):
            make(source, target, sems, c, p).start()
            return carry

        lax.fori_loop(1, devices, start, 0)
        own = pl.ds(pl.multiple_of(me * chunk, 8), chunk)
        target[c, own, :] = source[c, own, :]

    def receive(source, target, sems, c):
        def wait(p, carry):
            make(source, target, sems, c, p).wait()
            return carry

        lax.fori_loop(1, devices, wait, 0)

    for c in range(3):
        for p in range(1, rows):
            copy_row(c, p).wait()
        for z in range(zc):
            lines = jnp.concatenate([r1[c, r, pl.ds(z * ny, ny), :] for r in range(rows)], axis=0)
            modes = turn(dot(both[...], lines), 1.0)
            for k in range(kc):
                s2[c, pl.ds(z * jrows + k, devices, stride=chunk), :] = modes[k * devices:(k + 1) * devices]
        send(s2, r2, sem2, c)

    for c in range(3):
        receive(s2, r2, sem2, c)
        for k in range(kc):
            omega[c, k] = turn(dot(both[...], r2[c, pl.ds(k, n, stride=jrows), :]), 1.0)

    xi = lax.broadcasted_iota(jnp.int32, (n, n), 1)
    zi = lax.broadcasted_iota(jnp.int32, (n, n), 0)
    kx = jnp.where(xi < half, xi, xi - half).astype(jnp.float32)
    kz = jnp.where(zi < half, zi, zi - n).astype(jnp.float32)
    for c in range(3):
        for k in range(kc):
            yi = k * devices + me
            ky_int = yi - jnp.where(yi < half, 0, n)
            ky = jnp.full((n, n), ky_int, jnp.int32).astype(jnp.float32)
            if c == 0:
                square = kx * kx + ky * ky + kz * kz
                keep = (square > 0.0) & (zi != half) & (jnp.full((n, n), yi, jnp.int32) != half)
                factor[k] = jnp.where(keep, 1.0 / jnp.maximum(square, 1.0), 0.0) * (1.0 / (n * n * n))
                cross = ky * omega[2, k] - kz * omega[1, k]
            elif c == 1:
                cross = kz * omega[0, k] - kx * omega[2, k]
            else:
                cross = kx * omega[1, k] - ky * omega[0, k]
            hat = pltpu.roll(cross * factor[k], half, axis=1) * (-sign)
            s3[c, pl.ds(k, n, stride=jrows), :] = turn(dot(both[...], hat), -1.0)
        send(s3, r3, sem3, c)

    def copy_back(c, p):
        peer = lax.rem(row + p, rows)
        return pltpu.make_async_remote_copy(
            src_ref=w4.at[c, peer], dst_ref=r4.at[c, pl.ds(1 + row * zc, zc)], send_sem=sem4.at[0, c, p],
            recv_sem=sem4.at[1, c, p], device_id=(peer, col), device_id_type=MESH)

    def copy_layer(c, r, above):
        step, side = (1, 0) if above else (cols - 1, 1)
        return pltpu.make_async_remote_copy(
            src_ref=w4.at[c, r, zc - 1 if above else 0], dst_ref=r4.at[c, 0 if above else nz + 1],
            send_sem=sem4h.at[side, c, r], recv_sem=sem4h.at[side, c, rows],
            device_id=(r, lax.rem(col + step, cols)), device_id_type=MESH)

    for c in range(3):
        receive(s3, r3, sem3, c)
        for z in range(zc):
            modes = jnp.concatenate(
                [r3[c, pl.ds(z * jrows + k, devices, stride=chunk), :] for k in range(kc)], axis=0)
            lines = turn(dot(iy[...], modes), -1.0)
            for r in range(rows):
                w4[c, r, z] = lines[r * padded:(r + 1) * padded]

        for p in range(1, rows):
            copy_back(c, p).start()

        @pl.when(row == rows - 1)
        def _():
            for r in range(rows):
                copy_layer(c, r, True).start()

        @pl.when(row == 0)
        def _():
            for r in range(rows):
                copy_layer(c, r, False).start()

        r4[c, pl.ds(1 + row * zc, zc)] = w4[c, row]

    top = jnp.zeros((8, n), jnp.float32)
    for c in range(3):
        for p in range(1, rows):
            copy_back(c, p).wait()
        copy_layer(c, 0, True).wait_recv()
        copy_layer(c, 0, False).wait_recv()
        for z in range(nz + 2):
            product = dot(r4[c, z], bx[...])
            size = jnp.abs(product[:, 2 * n:])
            top = jnp.maximum(top, jnp.max(size.reshape(size.shape[0] // 8, 8, n), axis=0))
            for h in range(2):
                part = product[:, h * n:(h + 1) * n]
                fine[c * 2 + h, pl.ds(zp + z, ny, stride=zp), :] = part[:ny]
                fine[c * 2 + h, pl.ds(z, 1), :] = part[ny:ny + 1]
                fine[c * 2 + h, pl.ds((ny + 1) * zp + z, 1), :] = part[ny + 1:ny + 2]

    @pl.when(row == rows - 1)
    def _():
        for c in range(3):
            for r in range(rows):
                copy_layer(c, r, True).wait_send()

    @pl.when(row == 0)
    def _():
        for c in range(3):
            for r in range(rows):
                copy_layer(c, r, False).wait_send()

    peaks[me] = top

    def send_peak(p):
        return pltpu.make_async_remote_copy(
            src_ref=peaks.at[me], dst_ref=peaks.at[me], send_sem=semp.at[0, p], recv_sem=semp.at[1, p],
            device_id=where_is(lax.rem(me + p, devices)), device_id_type=MESH)

    def peak_start(p, carry):
        send_peak(p).start()
        return carry

    def peak_wait(p, carry):
        send_peak(p).wait()
        return carry

    lax.fori_loop(1, devices, peak_start, 0)

    def clear(y, carry):
        acc[y] = jnp.zeros((nzf, 2 * n), jnp.float32)
        return carry

    lax.fori_loop(0, nf + 6, clear, 0)
    lax.fori_loop(1, devices, peak_wait, 0)
    scale = COURANT / (jnp.max(peaks[...]) + EPSILON)

    def sweep(j):
        def plane(ch, y):
            return fine[ch, pl.ds(pl.multiple_of(y * zp, 8), zp), :]

        for c in range(3):
            for h in range(2):
                middle = plane(c * 2 + h, j + 1) * (0.75 * scale)
                for side in range(2):
                    line = middle + plane(c * 2 + h, j + 2 * side) * (0.25 * scale)
                    inner = 0.75 * line[1:nz + 1]
                    pack[side * 6 + c * 2 + h, pl.ds(0, nz, stride=2), :] = inner + 0.25 * line[0:nz]
                    pack[side * 6 + c * 2 + h, pl.ds(1, nz, stride=2), :] = inner + 0.25 * line[2:nz + 2]
        for side in range(2):
            y = 2 * j + side
            dx, dy, dz = [
                jnp.concatenate([pack[side * 6 + c * 2], pack[side * 6 + c * 2 + 1]], axis=1) for c in range(3)]
            disp_z[y] = dz
            parts = spread(scalar[y], dx)
            swept = parts[0]
            for offset in (1, 2, 3):
                swept = swept + pltpu.roll(parts[offset], offset, axis=1)
                swept = swept + pltpu.roll(parts[-offset], 2 * n - offset, axis=1)
            parts = spread(swept, dy)
            for offset in range(-3, 4):
                acc[y + 3 + offset] += parts[offset]

    def edge(i):
        return jnp.where(i < 2, i, ny - 4 + i)

    def sweep_edge(i, carry):
        sweep(edge(i))
        return carry

    def sweep_inner(j, carry):
        sweep(j)
        return carry

    lax.fori_loop(0, 4, sweep_edge, 0)

    def copy_y(up):
        step = 1 if up else rows - 1
        side = 0 if up else 1
        return pltpu.make_async_remote_copy(
            src_ref=acc.at[pl.ds(nf + 3 if up else 0, 3)], dst_ref=halo_y.at[side], send_sem=semy.at[0, side],
            recv_sem=semy.at[1, side], device_id=(lax.rem(row + step, rows), col), device_id_type=MESH)

    copy_y(True).start()
    copy_y(False).start()
    lax.fori_loop(2, ny - 2, sweep_inner, 0)

    row_of = lax.broadcasted_iota(jnp.int32, (nzf, 2 * n), 0)
    row8 = lax.broadcasted_iota(jnp.int32, (8, 2 * n), 0)

    def lift(p):
        tiles = []
        for side in range(2):
            y = 2 * p + side
            parts = spread(acc[y + 3], disp_z[y])
            kept = parts[0]
            above = jnp.zeros((8, 2 * n), jnp.float32)
            below = jnp.zeros((8, 2 * n), jnp.float32)
            for offset in (1, 2, 3):
                moved = pltpu.roll(parts[offset], offset, axis=0)
                kept = kept + jnp.where(row_of >= offset, moved, 0.0)
                above = above + jnp.where(row8 < offset, moved[:8], 0.0)
                moved = pltpu.roll(parts[-offset], nzf - offset, axis=0)
                kept = kept + jnp.where(row_of < nzf - offset, moved, 0.0)
                below = below + jnp.where(row8 >= 8 - offset, moved[nzf - 8:], 0.0)
            out[y] = kept
            tiles.append((above, below))
        zr[p] = tiles[0][0] + pltpu.roll(tiles[1][0], 4, axis=0)
        zl[p] = tiles[0][1] + pltpu.roll(tiles[1][1], 4, axis=0)

    def lift_inner(p, carry):
        lift(p)
        return carry

    def lift_edge(i, carry):
        lift(edge(i))
        return carry

    def copy_z(index):
        start, count = ((2, ny - 4), (0, 2), (ny - 2, 2))[index]
        here = pl.ds(start, count)
        return [
            pltpu.make_async_remote_copy(
                src_ref=source.at[here], dst_ref=target.at[here], send_sem=semz.at[0, side, index],
                recv_sem=semz.at[1, side, index], device_id=(row, lax.rem(col + step, cols)), device_id_type=MESH)
            for side, source, target, step in ((0, zr, zin_r, 1), (1, zl, zin_l, cols - 1))]

    lax.fori_loop(2, ny - 2, lift_inner, 0)
    for copy in copy_z(0):
        copy.start()
    copy_y(True).wait()
    copy_y(False).wait()
    for i in range(3):
        acc[3 + i] += halo_y[0, i]
        acc[nf + i] += halo_y[1, i]
    lax.fori_loop(0, 4, lift_edge, 0)
    for index in (1, 2):
        for copy in copy_z(index):
            copy.start()

    def finish(p, carry):
        low, high = zin_r[p], zin_l[p]
        for side in range(2):
            if side:
                low, high = pltpu.roll(low, 4, axis=0), pltpu.roll(high, 4, axis=0)
            out[2 * p + side, :8, :] += jnp.where(row8 < 3, low, 0.0)
            out[2 * p + side, nzf - 8:, :] += jnp.where(row8 >= 5, high, 0.0)
        return carry

    for index, (start, stop) in enumerate(((2, ny - 2), (0, 2), (ny - 2, ny))):
        for copy in copy_z(index):
            copy.wait()
        lax.fori_loop(start, stop, finish, 0)


def shards(rows, cols, vorticity, scalar):
    n = vorticity.shape[3]
    ny, nz = vorticity.shape[1], vorticity.shape[2]
    devices = rows * cols
    zc, kc = nz // rows, n // devices
    jrows = kc
    while zc * jrows % 8:
        jrows += 1
    padded = ny + 8
    zp = (nz + 2 + 7) // 8 * 8
    nf, nzf = 2 * ny, 2 * nz
    f32 = jnp.float32
    total = devices * zc * jrows
    vmem = pl.BlockSpec(memory_space=pltpu.VMEM)
    dma = pltpu.SemaphoreType.DMA
    return pl.pallas_call(
        functools.partial(body, rows, cols, jrows),
        out_shape=jax.ShapeDtypeStruct((nf, nzf, 2 * n), f32),
        in_specs=[vmem] * 6,
        out_specs=vmem,
        scratch_shapes=[
            pltpu.VMEM((3, ny * nz, n), f32),
            pltpu.VMEM((3, rows, zc * ny, n), f32),
            pltpu.VMEM((3, rows, zc * ny, n), f32),
            pltpu.VMEM((3, total, n), f32),
            pltpu.VMEM((3, total, n), f32),
            pltpu.VMEM((3, kc, n, n), f32),
            pltpu.VMEM((kc, n, n), f32),
            pltpu.VMEM((3, total, n), f32),
            pltpu.VMEM((3, total, n), f32),
            pltpu.VMEM((3, rows, zc, padded, n), f32),
            pltpu.VMEM((3, nz + 2, padded, n), f32),
            pltpu.VMEM((6, (ny + 2) * zp, n), f32),
            pltpu.VMEM((devices, 8, n), f32),
            pltpu.VMEM((12, nzf, n), f32),
            pltpu.VMEM((nf, nzf, 2 * n), f32),
            pltpu.VMEM((nf + 6, nzf, 2 * n), f32),
            pltpu.VMEM((2, 3, nzf, 2 * n), f32),
            pltpu.VMEM((ny, 8, 2 * n), f32),
            pltpu.VMEM((ny, 8, 2 * n), f32),
            pltpu.VMEM((ny, 8, 2 * n), f32),
            pltpu.VMEM((ny, 8, 2 * n), f32),
            dma((2, 3, rows)),
            dma((2, 3, devices)),
            dma((2, 3, devices)),
            dma((2, 3, rows)),
            dma((2, 3, rows + 1)),
            dma((2, devices)),
            dma((2, 2)),
            dma((2, 2, 3)),
        ],
        compiler_params=pltpu.CompilerParams(
            collective_id=0, has_side_effects=True, vmem_limit_bytes=56 * 1024 * 1024),
    )(vorticity.reshape(3, ny * nz, n), scalar, *[jnp.asarray(t) for t in tables(n, rows, padded)])


def solution(mesh):
    rows, cols = mesh.shape["row"], mesh.shape["col"]
    return jax.shard_map(
        functools.partial(shards, rows, cols),
        mesh=mesh,
        in_specs=(P(None, "row", "col", None), P("row", "col", None)),
        out_specs=P("row", "col", None),
        check_vma=False,
    )
```
